512 devices in a mesh: shift: 8 (over x, core), batch: 16 (over z), cols: 4 (over y).
Axes of the slice: x: 4, y: 4, z: 16, core: 2. Of those that a mesh axis runs over, the one named last changes fastest.
Arguments:
- partial_up: float32 [128, 768, 3072], P(('shift', 'batch'), None, 'cols'), parts along dimension 0, may hold values from -0.875 to 0.875
- partial_down: float32 [128, 3072, 768], P(('shift', 'batch'), 'cols'), parts along dimension 0, may hold values from -0.875 to 0.875
- partial_norm: float32 [128, 768], P(('shift', 'batch')), parts along dimension 0, may hold values from -8 to 8
- partial_bias: float32 [128, 768], P(('shift', 'batch')), parts along dimension 0, may hold values from -8 to 8
- master_up: float32 [6144, 3072], P(('shift', 'batch'), 'cols'), parts along dimension 0, may hold values from -0.21875 to 0.21875
- master_down: float32 [24576, 768], P(('shift', 'cols'), 'batch'), parts along dimension 0, may hold values from -0.109375 to 0.109375
- master_norm: float32 [6144], P(('shift', 'batch')), parts along dimension 0, may hold values from 0.25 to 1.75
- master_bias: float32 [6144], P(('shift', 'batch')), parts along dimension 0, may hold values from -3 to 3
- memory_up: float32 [6144, 3072], P(('shift', 'batch'), 'cols'), parts along dimension 0, may hold values from -1.75 to 1.75
- memory_down: float32 [24576, 768], P(('shift', 'cols'), 'batch'), parts along dimension 0, may hold values from -1.75 to 1.75
- memory_norm: float32 [6144], P(('shift', 'batch')), parts along dimension 0, may hold values from -1.75 to 1.75
- memory_bias: float32 [6144], P(('shift', 'batch')), parts along dimension 0, may hold values from -1.75 to 1.75
Outputs:
- compute_up: bfloat16 [6144, 3072], P('shift', 'cols'), parts along dimension 0
- compute_down: bfloat16 [24576, 768], P(('shift', 'cols')), parts along dimension 0
- compute_norm: bfloat16 [6144], P('shift'), parts along dimension 0
- compute_bias: bfloat16 [6144], P('shift'), parts along dimension 0
- stepped_up: float32 [6144, 3072], P(('shift', 'batch'), 'cols'), parts along dimension 0
- stepped_down: float32 [24576, 768], P(('shift', 'cols'), 'batch'), parts along dimension 0
- stepped_norm: float32 [6144], P(('shift', 'batch')), parts along dimension 0
- stepped_bias: float32 [6144], P(('shift', 'batch')), parts along dimension 0
- state_new_up: float32 [6144, 3072], P(('shift', 'batch'), 'cols'), parts along dimension 0
- state_new_down: float32 [24576, 768], P(('shift', 'cols'), 'batch'), parts along dimension 0
- state_new_norm: float32 [6144], P(('shift', 'batch')), parts along dimension 0
- state_new_bias: float32 [6144], P(('shift', 'batch')), parts along dimension 0
The draws below stay inside these ranges and needn't reach their ends.
There are 8 independent parts, one for each index of `shift`. The reference program is written for one: setup_inputs(seed, part) draws one part's arguments, and reference() takes and returns one part's arrays. A program takes and returns all parts, laid end to end along the dimension named above; each array names one. Nothing has to cross between parts.
All inputs are finite; a program needn't handle non-finite values.
Results may differ from the reference program's by a relative error of at most 0.0085.
Values may be sent and summed in bfloat16 or wider, within the bound.
No kernel may reach another device: no remote copies, remote signals or barrier semaphores. Data moves between devices by JAX's collectives and lax.ppermute only.
A program may use at most 64 MiB of HBM per device.

```python
import jax
import jax.numpy as jnp

WIDTH = 768
INNER = 3072
REPLICAS = 16


def raised(drawn, rng, source, target, parts, factor):
    def block_of(position):
        return (jnp.arange(drawn.shape[position]) // (drawn.shape[position] // parts)).reshape((-1,) + (1,) * (drawn.ndim - 1 - position))

    first = jax.random.permutation(rng, parts)[block_of(target)]
    second = (block_of(target) + parts // 2) % parts
    return jnp.where((block_of(source) == first) | (block_of(source) == second), factor * drawn, drawn)


def block_scale(key, shape, shards, low, largest):
    def one(position, parts):
        steps = jax.random.uniform(jax.random.fold_in(jax.random.fold_in(key, 6), position), (parts,), jnp.float32, low / len(shards), largest / len(shards))
        return jnp.repeat(jnp.exp(steps), shape[position] // parts).reshape((-1,) + (1,) * (len(shape) - position - 1))

    level = one(*shards[0])
    for cut in shards[1:]:
        level = level * one(*cut)
    return level


def noise(rng, shape, deviation, reach, pieces=(), held_as=jnp.bfloat16):
    drawn = deviation * jax.random.normal(rng, shape, jnp.float32)
    if pieces:
        drawn = drawn * block_scale(rng, shape, pieces, -0.22, 0.18)
    return jnp.clip(drawn, -reach, reach).astype(held_as)


def noise_with(key, shape, scale, most, split, heavy, dtype=jnp.bfloat16):
    values = scale * jax.random.normal(key, shape, jnp.float32)
    if split:
        values = values * block_scale(key, shape, split, -0.22, 0.18)
    return jnp.clip(raised(values, jax.random.fold_in(key, 3), *heavy), -most, most).astype(dtype)


def setup_inputs(seed: int = 0, part: int = 0) -> dict:
    arg_keys = jax.random.split(jax.random.key(seed), 13)
    part_keys = jax.random.split(jax.random.fold_in(arg_keys[12], part), 13)
    return {
        "partial_up": noise_with(part_keys[0], (REPLICAS, WIDTH, INNER), 0.1, 0.875, ((0, 16), (2, 4)), (0, 1, 16, 2.0), jnp.float32),
        "partial_down": noise_with(part_keys[1], (REPLICAS, INNER, WIDTH), 0.1, 0.875, ((0, 16), (1, 4)), (0, 2, 16, 2.0), jnp.float32),
        "partial_norm": noise_with(part_keys[2], (REPLICAS, WIDTH), 1.0, 8.0, ((0, 16),), (0, 1, 16, 2.0), jnp.float32),
        "partial_bias": noise_with(part_keys[3], (REPLICAS, WIDTH), 1.0, 8.0, ((0, 16),), (0, 1, 16, 2.0), jnp.float32),
        "master_up": noise(part_keys[4], (WIDTH, INNER), WIDTH ** -0.5, 0.21875, ((0, 16), (1, 4)), jnp.float32),
        "master_down": noise(part_keys[5], (INNER, WIDTH), INNER ** -0.5, 0.109375, ((0, 4), (1, 16)), jnp.float32),
        "master_norm": jnp.clip(1.0 + 0.15 * jax.random.normal(part_keys[6], (WIDTH,), jnp.float32), 0.25, 1.75),
        "master_bias": noise(part_keys[7], (WIDTH,), 0.5, 3.0, ((0, 16),), jnp.float32),
        "memory_up": noise(part_keys[8], (WIDTH, INNER), 0.3, 1.75, ((0, 16), (1, 4)), jnp.float32),
        "memory_down": noise(part_keys[9], (INNER, WIDTH), 0.3, 1.75, ((0, 4), (1, 16)), jnp.float32),
        "memory_norm": noise(part_keys[10], (WIDTH,), 0.3, 1.75, ((0, 16),), jnp.float32),
        "memory_bias": noise(part_keys[11], (WIDTH,), 0.3, 1.75, ((0, 16),), jnp.float32),
    }


learn_rate = 0.1
hold_rate = 0.8


def reference(partial_up, partial_down, partial_norm, partial_bias, master_up, master_down, master_norm, master_bias, memory_up, memory_down, memory_norm, memory_bias):
    mean_up = jnp.sum(partial_up.astype(jnp.float32), axis=0) * REPLICAS ** -0.5
    mean_down = jnp.sum(partial_down.astype(jnp.float32), axis=0) * REPLICAS ** -0.5
    mean_norm = jnp.sum(partial_norm.astype(jnp.float32), axis=0) * REPLICAS ** -0.5
    mean_bias = jnp.sum(partial_bias.astype(jnp.float32), axis=0) * REPLICAS ** -0.5
    state_new_up = hold_rate * memory_up + mean_up
    stepped_up = master_up - learn_rate * state_new_up
    state_new_down = hold_rate * memory_down + mean_down
    stepped_down = master_down - learn_rate * state_new_down
    state_new_norm = hold_rate * memory_norm + mean_norm
    stepped_norm = master_norm - learn_rate * state_new_norm
    state_new_bias = hold_rate * memory_bias + mean_bias
    stepped_bias = master_bias - learn_rate * state_new_bias
    compute_up = stepped_up.astype(jnp.bfloat16)
    compute_down = stepped_down.astype(jnp.bfloat16)
    compute_norm = stepped_norm.astype(jnp.bfloat16)
    compute_bias = stepped_bias.astype(jnp.bfloat16)
    return compute_up, compute_down, compute_norm, compute_bias, stepped_up, stepped_down, stepped_norm, stepped_bias, state_new_up, state_new_down, state_new_norm, state_new_bias
```

```python
import jax
import jax.numpy as jnp
from jax import lax
from jax.sharding import PartitionSpec as P

learn_rate = 0.1
hold_rate = 0.8
up_cuts = [24] * 32
down_cuts = [24] * 30 + [16] * 3


def pieces_of(array, cuts):
    at, pieces = 0, []
    for rows in cuts:
        pieces.append(lax.slice_in_dim(array, at, at + rows))
        at += rows
    return pieces


def on_device(
    partial_up,
    partial_down,
    partial_norm,
    partial_bias,
    master_up,
    master_down,
    master_norm,
    master_bias,
    memory_up,
    memory_down,
    memory_norm,
    memory_bias,
):
    place = lax.axis_index("batch")
    share = master_norm.shape[0]
    mean_rate = lax.axis_size("batch") ** (-0.5)
    kept_rate = learn_rate * hold_rate
    moved_rate = learn_rate * mean_rate

    def kept(master, memory):
        return (master - kept_rate * memory).astype(jnp.bfloat16)

    kept_here = jnp.concatenate([kept(master_up, memory_up), kept(master_down.T, memory_down.T)])
    kept_here, partial_up, partial_down, partial_norm, partial_bias = lax.optimization_barrier(
        (kept_here, partial_up, partial_down, partial_norm, partial_bias)
    )
    kept_all = lax.all_gather(kept_here, "batch")

    def in_place(part):
        whole = jnp.zeros((share * lax.axis_size("batch"),), jnp.bfloat16)
        return lax.dynamic_update_slice_in_dim(whole, part, place * share, 0)

    vectors = jnp.concatenate(
        [
            partial_norm[0].astype(jnp.bfloat16),
            partial_bias[0].astype(jnp.bfloat16),
            in_place(kept(master_norm, memory_norm)),
            in_place(kept(master_bias, memory_bias)),
        ]
    ).reshape(-1, 128)
    ups = pieces_of(partial_up[0].astype(jnp.bfloat16), up_cuts)
    downs = pieces_of(partial_down[0].astype(jnp.bfloat16), down_cuts)
    sums = lax.psum((*ups, *downs, vectors), "batch")
    sum_up = jnp.concatenate(sums[: len(ups)])
    sum_down = jnp.concatenate(sums[len(ups) : -1])
    sum_norm, sum_bias, kept_norm, kept_bias = jnp.split(sums[-1].reshape(-1), 4)
    kept_up = kept_all[:, :share].reshape(sum_up.shape)
    kept_down = kept_all[:, share:].reshape(sum_down.shape).T

    def next_compute(kept, total):
        return (kept.astype(jnp.float32) - moved_rate * total.astype(jnp.float32)).astype(jnp.bfloat16)

    def next_state(master, memory, total, dim):
        here = lax.dynamic_slice_in_dim(total, place * share, share, dim).astype(jnp.float32)
        state = hold_rate * memory + mean_rate * here
        return master - learn_rate * state, state

    stepped_up, state_up = next_state(master_up, memory_up, sum_up, 0)
    stepped_down, state_down = next_state(master_down, memory_down, sum_down, 1)
    stepped_norm, state_norm = next_state(master_norm, memory_norm, sum_norm, 0)
    stepped_bias, state_bias = next_state(master_bias, memory_bias, sum_bias, 0)
    return (
        next_compute(kept_up, sum_up),
        next_compute(kept_down, sum_down),
        next_compute(kept_norm, sum_norm),
        next_compute(kept_bias, sum_bias),
        stepped_up,
        stepped_down,
        stepped_norm,
        stepped_bias,
        state_up,
        state_down,
        state_norm,
        state_bias,
    )


def solution(mesh):
    return jax.shard_map(
        on_device,
        mesh=mesh,
        in_specs=(
            P(("shift", "batch"), None, "cols"),
            P(("shift", "batch"), "cols", None),
            P(("shift", "batch"), None),
            P(("shift", "batch"), None),
            P(("shift", "batch"), "cols"),
            P(("shift", "cols"), "batch"),
            P(("shift", "batch")),
            P(("shift", "batch")),
            P(("shift", "batch"), "cols"),
            P(("shift", "cols"), "batch"),
            P(("shift", "batch")),
            P(("shift", "batch")),
        ),
        out_specs=(
            P("shift", "cols"),
            P(("shift", "cols"), None),
            P("shift"),
            P("shift"),
            P(("shift", "batch"), "cols"),
            P(("shift", "cols"), "batch"),
            P(("shift", "batch")),
            P(("shift", "batch")),
            P(("shift", "batch"), "cols"),
            P(("shift", "cols"), "batch"),
            P(("shift", "batch")),
            P(("shift", "batch")),
        ),
        check_vma=False,
    )
```
